32 devices in a mesh: obs: 8 (over z, y), chan: 4 (over x, core).
Axes of the slice: x: 2, y: 2, z: 4, core: 2. Of those that a mesh axis runs over, the one named last changes fastest.
Arguments:
- jacobian: bfloat16 [2048, 128, 137], P('obs', 'chan'), may hold values from -0.5 to 0.5
- departures: float32 [128, 2048], P('chan', 'obs'), may hold values from -6 to 6
- obs_weights: float32 [128, 2048], P('chan', 'obs'), may hold values from 0.25 to 4
- column_count: int32 [8], P('obs'), may hold values from 1 to 256, as said below
- grid_block: int32 [16], P('obs'), may hold values from 0 to 15, as said below
- sqrt_cov: float32 [137, 137], replicated, may hold values from -0.5 to 0.5
Outputs:
- increment: float32 [2048, 137], P('obs')
- residual: float32 [2048, 137], P('obs')
The draws below stay inside these ranges and needn't reach their ends.
Inputs may be any that keep to these rules, and one draw needn't show every extreme that they name: The first column_count of a device's 256 column slots are observed; some device has all 256 observed in every draw. `grid_block`: the owner of grid block g is index g // 2 of obs. The 2 blocks of one device match blocks of 2 different owners; in every draw some owner has a block matched by each device (every device matches one of that owner's blocks), and some device matches that owner's last block.
All inputs are finite; a program needn't handle non-finite values.
Results may differ from the reference program's by a relative error of at most 0.02.
Values may be sent and summed in bfloat16 or wider, within the bound.
A program may use at most 64 MiB of HBM per device.

```python
import math
import jax
import jax.numpy as jnp
from jax import lax

L = 137
BLOCK = 128
ITERS = 5
OBS_BLK = 2
GRID_BLK = 2
CHANNELS = 128
COLS = 2048
N_OBS = 8


def draw_column_count(key, part):
    span = OBS_BLK * BLOCK
    drawn = jax.random.randint(jax.random.fold_in(key, 11), (N_OBS,), 0, span + 1)
    counts = jnp.maximum(drawn * drawn // span, 1)
    fullest = jax.random.randint(jax.random.fold_in(key, 12), (), 0, N_OBS)
    counts = jnp.where(jnp.arange(N_OBS) == fullest, span, counts)
    return counts.astype(jnp.int32)


def draw_grid_block(key, part):
    common = jax.random.randint(jax.random.fold_in(key, 21), (), 0, N_OBS)
    scores = jax.random.randint(jax.random.fold_in(key, 22), (N_OBS, N_OBS), 0, 1048576)
    scores = scores * N_OBS + jnp.arange(N_OBS)[None, :]
    scores = jnp.where(jnp.arange(N_OBS)[None, :] == common, -1, scores)
    owners = jnp.argsort(scores, axis=1, stable=True)[:, :OBS_BLK]
    places = jax.random.randint(jax.random.fold_in(key, 23), (N_OBS, OBS_BLK), 0, GRID_BLK)
    chosen = jax.random.randint(jax.random.fold_in(key, 24), (), 0, N_OBS)
    rows = jnp.arange(N_OBS)[:, None]
    slots = jnp.arange(OBS_BLK)[None, :]
    places = jnp.where((rows == chosen) & (slots == 0), GRID_BLK - 1, places)
    return (owners * GRID_BLK + places).reshape(-1).astype(jnp.int32)


def steps_of(rng, extent, cuts, least, high):
    factor_of = 1.0
    for dim, blocks in cuts:
        draws = jax.random.uniform(jax.random.fold_in(jax.random.fold_in(rng, 6), dim), (blocks,), jnp.float32, least / len(cuts), high / len(cuts))
        factor_of = factor_of * jnp.repeat(jnp.exp(draws), extent[dim] // blocks).reshape((-1,) + (1,) * (len(extent) - 1 - dim))
    return factor_of


def scatter_about(stream_key, shape, scale, bound, cuts=(), held_as=jnp.bfloat16):
    result = scale * jax.random.normal(stream_key, shape, jnp.float32)
    if cuts:
        result = result * steps_of(stream_key, shape, cuts, -0.22, 0.18)
    return jnp.clip(result, -bound, bound).astype(held_as)


def setup_inputs(seed: int = 0) -> dict:
    arg_keys = jax.random.split(jax.random.key(seed), 7)
    jacobian = scatter_about(arg_keys[0], (COLS, CHANNELS, L), L ** -0.5, 0.5, ((0, 8), (1, 4)))
    departures = scatter_about(arg_keys[1], (CHANNELS, COLS), 1.0, 6.0, ((0, 4), (1, 8)), jnp.float32)
    obs_weights = jnp.clip(jnp.exp(math.log(4.0) - 2.7725887 * jax.random.uniform(arg_keys[2], (CHANNELS, COLS), jnp.float32) ** steps_of(arg_keys[2], (CHANNELS, COLS), ((0, 4), (1, 8)), -0.2, 0.2)), 0.25, 4.0)
    column_count = draw_column_count(jax.random.fold_in(arg_keys[6], 71), 0)
    grid_block = draw_grid_block(jax.random.fold_in(arg_keys[6], 71), 0)
    sqrt_cov = scatter_about(arg_keys[5], (L, L), L ** -0.5, 0.5, (), jnp.float32)
    return {"jacobian": jacobian, "departures": departures, "obs_weights": obs_weights, "column_count": column_count, "grid_block": grid_block, "sqrt_cov": sqrt_cov}


def source_block(operands):
    jac_part, weight_part, mask_part, depart_part = operands
    kernel = jac_part.astype(jnp.float32)
    scaled = (mask_part[:, None] * weight_part * depart_part).astype(jnp.bfloat16)
    scaled = lax.optimization_barrier(scaled).astype(jnp.float32)
    return jnp.einsum('cnl,cn->cl', kernel, scaled, precision=lax.Precision.HIGHEST)

def normal_block(operands):
    jac_part, weight_part, mask_part, field_part = operands
    kernel = jac_part.astype(jnp.float32)
    predicted = jnp.einsum('cnl,cl->cn', kernel, field_part.astype(jnp.float32), precision=lax.Precision.HIGHEST)
    scaled = (mask_part[:, None] * weight_part * predicted).astype(jnp.bfloat16)
    scaled = lax.optimization_barrier(scaled).astype(jnp.float32)
    return jnp.einsum('cnl,cn->cl', kernel, scaled, precision=lax.Precision.HIGHEST)

def reference(jacobian, departures, obs_weights, column_count, grid_block, sqrt_cov):
    columns_all = jacobian.shape[0]
    per_device = OBS_BLK * BLOCK
    position = jnp.arange(columns_all, dtype=jnp.int32)
    observed = (position % per_device < column_count[position // per_device]).astype(jnp.float32)
    block_total = columns_all // BLOCK
    jac_blocks = jacobian.reshape(block_total, BLOCK, CHANNELS, L)
    weight_blocks = obs_weights.T.reshape(block_total, BLOCK, CHANNELS)
    depart_blocks = departures.T.reshape(block_total, BLOCK, CHANNELS)
    mask_blocks = observed.reshape(block_total, BLOCK)
    grid_total = GRID_BLK * N_OBS

    def collect(terms):
        summed = jnp.zeros((grid_total, BLOCK, L), jnp.float32).at[grid_block].add(terms)
        return summed.reshape(grid_total * BLOCK, L)

    def spread(field):
        return jnp.dot(field, sqrt_cov, precision=lax.Precision.HIGHEST)

    def spread_back(field):
        return jnp.dot(field, sqrt_cov.T, precision=lax.Precision.HIGHEST)

    def normal(direction):
        rounded = lax.optimization_barrier(spread(direction).astype(jnp.bfloat16))
        fields = rounded.reshape(grid_total, BLOCK, L)[grid_block]
        terms = lax.map(normal_block, (jac_blocks, weight_blocks, mask_blocks, fields))
        return direction + spread_back(collect(terms))
    source_terms = lax.map(source_block, (jac_blocks, weight_blocks, mask_blocks, depart_blocks))
    residual = spread_back(collect(source_terms))
    control = jnp.zeros_like(residual)
    direction = residual
    norm_now = jnp.sum(residual * residual)
    for iteration in range(ITERS):
        image = normal(direction)
        step_length = norm_now / jnp.sum(direction * image)
        control = control + step_length * direction
        residual = residual - step_length * image
        norm_next = jnp.sum(residual * residual)
        direction = residual + norm_next / norm_now * direction
        norm_now = norm_next
    return (spread(control), residual)
```

```python
import functools
import jax
import jax.numpy as jnp
from jax import lax
from jax.experimental import pallas as pl
from jax.experimental.pallas import tpu as pltpu
from jax.sharding import PartitionSpec as P

BLOCK = 128
ITERS = 5
GRID_BLK = 2
HIGHEST = lax.Precision.HIGHEST
MESH = pl.DeviceIdType.MESH


def block_terms(jac_part, weight_part, mask_part, predicted):
    scaled = (mask_part[:, None] * weight_part * predicted).astype(jnp.bfloat16)
    return lax.dot_general(
        jac_part, scaled, (((1,), (1,)), ((0,), (0,))), preferred_element_type=jnp.float32
    )


def forward_terms(jac_part, weight_part, mask_part, field_part):
    predicted = lax.dot_general(
        jac_part, field_part, (((2,), (1,)), ((0,), (0,))), preferred_element_type=jnp.float32
    )
    return block_terms(jac_part, weight_part, mask_part, predicted)


def exchange_per_step(jacobian, departures, obs_weights, column_count, grid_block, sqrt_cov):
    obs_count = lax.axis_size("obs")
    myself = lax.axis_index("obs")
    capacity, group_channels, layers = jacobian.shape
    block_count = capacity // BLOCK
    weight_cols = obs_weights.T
    depart_cols = departures.T
    observed = (jnp.arange(capacity, dtype=jnp.int32) < column_count[0]).astype(jnp.float32)
    every_id = lax.all_gather(grid_block, "obs", axis=0, tiled=True).reshape(obs_count, block_count)
    targets = jnp.arange(obs_count, dtype=jnp.int32)
    send_pick = (grid_block[None, :] // GRID_BLK == targets[:, None]).astype(jnp.float32)
    owned_here = every_id // GRID_BLK == myself
    places = every_id % GRID_BLK
    grid_index = jnp.arange(GRID_BLK, dtype=jnp.int32)
    take_pick = jnp.sum(
        ((places[None] == grid_index[:, None, None]) & owned_here[None]).astype(jnp.float32), axis=2
    )
    share_cols = BLOCK

    def local_terms(kernel_fn, inputs):
        return kernel_fn(jacobian, weight_cols, observed, inputs)

    def to_owners(terms):
        blocked = terms.reshape(block_count, BLOCK, layers)
        blocked = lax.psum(blocked, "chan")
        outgoing = jnp.dot(
            send_pick, blocked.reshape(block_count, -1), precision=lax.Precision.HIGHEST
        )
        incoming = lax.all_to_all(
            outgoing.reshape(obs_count, share_cols, layers),
            "obs",
            split_axis=0,
            concat_axis=0,
            tiled=True,
        )
        summed = jnp.dot(
            take_pick, incoming.reshape(obs_count, -1), precision=lax.Precision.HIGHEST
        )
        return summed.reshape(GRID_BLK, share_cols, layers)

    def spread(field):
        return jnp.dot(
            field.reshape(-1, layers), sqrt_cov, precision=lax.Precision.HIGHEST
        ).reshape(field.shape)

    def spread_back(field):
        flat = lax.dot_general(
            field.reshape(-1, layers),
            sqrt_cov,
            (((1,), (1,)), ((), ())),
            precision=lax.Precision.HIGHEST,
        )
        return flat.reshape(field.shape)

    def squared(values):
        partial_sum = jnp.sum(values * values)
        return lax.psum(partial_sum, "obs")

    residual = spread_back(to_owners(local_terms(block_terms, depart_cols)))
    control = jnp.zeros_like(residual)
    direction = residual
    norm_now = squared(residual)
    for iteration in range(ITERS):
        rounded = spread(direction).astype(jnp.bfloat16).reshape(GRID_BLK, -1)
        to_outgoing = jnp.dot(
            take_pick.T.astype(jnp.bfloat16), rounded, preferred_element_type=jnp.float32
        ).astype(jnp.bfloat16)
        to_incoming = lax.all_to_all(
            to_outgoing.reshape(obs_count, share_cols, layers),
            "obs",
            split_axis=0,
            concat_axis=0,
            tiled=True,
        )
        picked = jnp.dot(
            send_pick.T.astype(jnp.bfloat16),
            to_incoming.reshape(obs_count, -1),
            preferred_element_type=jnp.float32,
        )
        picked = picked.astype(jnp.bfloat16).reshape(block_count, share_cols, layers)
        fetched = picked.reshape(capacity, layers)
        image = direction + spread_back(to_owners(local_terms(forward_terms, fetched)))
        curvature_partial_sum = jnp.sum(direction * image)
        step_length = norm_now / lax.psum(curvature_partial_sum, "obs")
        control = control + step_length * direction
        residual = residual - step_length * image
        norm_next = squared(residual)
        direction = residual + norm_next / norm_now * direction
        norm_now = norm_next
    increment = spread(control)
    return (increment.reshape(-1, layers), residual.reshape(-1, layers))


def cg_kernel(
    obs_count, chan_count, jac_ref, gram_ref, cov_ref, pick_ref, take_ref, increment_ref,
    residual_ref, weight_ref, parts_ref, back_ref, sum_send, sum_recv, back_send, back_recv
):
    device_count = obs_count * chan_count
    me = lax.axis_index("obs") * chan_count + lax.axis_index("chan")
    rows, padded, lanes = jac_ref.shape
    layers = increment_ref.shape[1]
    share = BLOCK // device_count
    grid_cols = take_ref.shape[1]
    piece = GRID_BLK * share

    def coords(target):
        return (target // chan_count, target % chan_count)

    barrier = pltpu.get_barrier_semaphore()

    def greet(offset, carry):
        pl.semaphore_signal(
            barrier, inc=1, device_id=coords((me + offset) % device_count), device_id_type=MESH
        )
        return carry

    lax.fori_loop(1, device_count, greet, 0)

    def dot(a, b):
        return jnp.dot(a, b, precision=HIGHEST, preferred_element_type=jnp.float32)

    def source_step(n, acc):
        kernel = jac_ref[n].astype(jnp.float32)
        weight_ref[pl.ds(n, 1), :] = kernel[layers : layers + 1] + kernel[layers + 1 : layers + 2]
        return acc + kernel * kernel[layers + 2 : layers + 3]

    zero = jnp.zeros((padded, lanes), jnp.float32)
    residual = dot(lax.fori_loop(0, rows, source_step, zero, unroll=4), take_ref[...])

    control = direction = image = None
    norm_last = step_last = None
    for step in range(ITERS):
        spread = dot(gram_ref[...], residual)
        field = dot(spread, pick_ref[...])

        def normal_step(n, acc):
            kernel = jac_ref[n].astype(jnp.float32)
            predicted = jnp.sum(kernel * field, axis=0, keepdims=True)
            return acc + kernel * (predicted * weight_ref[pl.ds(n, 1), :])

        terms = lax.fori_loop(0, rows, normal_step, zero, unroll=4)
        applied = residual + dot(terms, take_ref[...])
        norm_part = jnp.sum(residual * spread, axis=0, keepdims=True)
        curve_part = jnp.sum(applied * spread, axis=0, keepdims=True)
        sub = lax.broadcasted_iota(jnp.int32, (8, grid_cols), 0)
        both = jnp.where(sub == 0, norm_part, jnp.where(sub == 1, curve_part, 0.0))
        if grid_cols < 128:
            both = jnp.concatenate([both, jnp.zeros((8, 128 - grid_cols), jnp.float32)], axis=1)
        parts_ref[step, me] = both
        if step == 0:
            pl.semaphore_wait(barrier, device_count - 1)

        def send_sum(offset, carry, step=step):
            pltpu.make_async_remote_copy(
                src_ref=parts_ref.at[step, me],
                dst_ref=parts_ref.at[step, me],
                send_sem=sum_send.at[step],
                recv_sem=sum_recv.at[step],
                device_id=coords((me + offset) % device_count),
                device_id_type=MESH,
            ).start()
            return carry

        lax.fori_loop(1, device_count, send_sum, 0)
        others = parts_ref.at[step, pl.ds(0, device_count - 1)]
        pltpu.make_async_copy(others, others, sum_recv.at[step]).wait()
        pltpu.make_async_copy(others, others, sum_send.at[step]).wait()
        total = jnp.sum(jnp.sum(parts_ref[step], axis=0), axis=1, keepdims=True)
        norm_now, curve = total[0:1], total[1:2]
        if step == 0:
            length = norm_now / curve
            direction, image = residual, applied
            control = length * direction
        else:
            ratio = norm_now / norm_last
            length = norm_now / (curve - ratio * norm_now / step_last)
            direction = residual + ratio * direction
            image = applied + ratio * image
            control = control + length * direction
        residual = residual - length * image
        norm_last, step_last = norm_now, length

    def turned(a, b):
        return lax.dot_general(
            a, b, (((0,), (0,)), ((), ())), precision=HIGHEST, preferred_element_type=jnp.float32
        )

    outs = (turned(control, gram_ref[...]), turned(residual, cov_ref[...]))
    out_stage, landed = back_ref.at[0], back_ref.at[1]
    for which, value in enumerate(outs):
        for owner in range(obs_count):
            out_stage[owner * chan_count, which, :, :] = value[owner * piece : (owner + 1) * piece, :layers]
    landed[me] = out_stage[(me // chan_count) * chan_count]

    def send_back(offset, carry):
        target = (me + offset) % device_count
        pltpu.make_async_remote_copy(
            src_ref=out_stage.at[(target // chan_count) * chan_count],
            dst_ref=landed.at[me],
            send_sem=back_send,
            recv_sem=back_recv,
            device_id=coords(target),
            device_id_type=MESH,
        ).start()
        return carry

    lax.fori_loop(1, device_count, send_back, 0)
    others = landed.at[pl.ds(0, device_count - 1)]
    pltpu.make_async_copy(others, others, back_recv).wait()
    pltpu.make_async_copy(others, others, back_send).wait()
    for which, out_ref in enumerate((increment_ref, residual_ref)):
        for block in range(GRID_BLK):
            for source in range(device_count):
                first = block * BLOCK + source * share
                out_ref[first : first + share, :] = landed[
                    source, which, block * share : (block + 1) * share, :
                ]


def shared_columns(jacobian, departures, obs_weights, column_count, grid_block, sqrt_cov):
    obs_count, chan_count = lax.axis_size("obs"), lax.axis_size("chan")
    device_count = obs_count * chan_count
    capacity, group_channels, layers = jacobian.shape
    block_count = capacity // BLOCK
    share = BLOCK // device_count
    padded = -(-(layers + 3) // 16) * 16
    cols = obs_count * block_count * share
    halves = 1
    while halves * 2 * cols <= 128 and chan_count % (halves * 2) == 0:
        halves *= 2
    grid_total = GRID_BLK * obs_count

    observed = (jnp.arange(capacity, dtype=jnp.int32) < column_count[0]).astype(jnp.float32)
    weight = observed[:, None] * obs_weights.T
    weight_high = weight.astype(jnp.bfloat16)
    weight_low = (weight - weight_high.astype(jnp.float32)).astype(jnp.bfloat16)
    source = (weight * departures.T).astype(jnp.bfloat16)
    extra = jnp.stack([weight_high, weight_low, source], axis=2)
    packed = jnp.concatenate([jacobian, extra], axis=2)
    packed = jnp.pad(packed, ((0, 0), (0, 0), (0, padded - layers - 3)))
    packed = packed.reshape(block_count, device_count, share * group_channels * padded)
    packed = packed.transpose(1, 0, 2).reshape(device_count, -1, 128)
    packed = lax.all_to_all(packed, ("obs", "chan"), split_axis=0, concat_axis=0, tiled=True)
    packed = packed.reshape(
        obs_count, halves, chan_count // halves, block_count * share, group_channels, padded
    )
    jac = packed.transpose(2, 4, 5, 1, 0, 3).reshape(-1, padded, halves * cols)

    every_id = lax.all_gather(grid_block, "obs", axis=0, tiled=True)
    hit = every_id[:, None] == jnp.arange(grid_total, dtype=jnp.int32)[None, :]
    same = jnp.eye(share, dtype=jnp.bool_)
    take = (hit[:, None, :, None] & same[None, :, None, :]).astype(jnp.float32)
    take = take.reshape(cols, grid_total * share)
    take = jnp.concatenate([take] * halves, axis=0)
    fill = padded - layers
    gram = jnp.dot(sqrt_cov.T, sqrt_cov, precision=HIGHEST)
    gram = jnp.pad(gram, ((0, fill), (0, fill)))
    cov = jnp.pad(sqrt_cov.T, ((0, fill), (0, fill)))

    out = jax.ShapeDtypeStruct((GRID_BLK * BLOCK, layers), jnp.float32)
    vmem = pl.BlockSpec(memory_space=pltpu.VMEM)
    return pl.pallas_call(
        functools.partial(cg_kernel, obs_count, chan_count),
        out_shape=(out, out),
        in_specs=[vmem] * 5,
        out_specs=(vmem, vmem),
        scratch_shapes=[
            pltpu.VMEM((jac.shape[0], jac.shape[2]), jnp.float32),
            pltpu.VMEM((ITERS, device_count, 8, 128), jnp.float32),
            pltpu.VMEM((2, device_count, 2, GRID_BLK * share, layers), jnp.float32),
            pltpu.SemaphoreType.DMA((ITERS,)),
            pltpu.SemaphoreType.DMA((ITERS,)),
            pltpu.SemaphoreType.DMA,
            pltpu.SemaphoreType.DMA,
        ],
        compiler_params=pltpu.CompilerParams(collective_id=0, has_side_effects=True),
    )(jac, gram, cov, take.T, take)


def solution(mesh):
    device_count = mesh.shape["obs"] * mesh.shape["chan"]
    plan = shared_columns if BLOCK % device_count == 0 else exchange_per_step
    in_specs = (P("obs", "chan", None), P("chan", "obs"), P("chan", "obs"), P("obs"), P("obs"), P())
    out_specs = (P("obs", None), P("obs", None))
    return jax.shard_map(plan, mesh=mesh, in_specs=in_specs, out_specs=out_specs, check_vma=False)
```

```python
import functools
import jax
import jax.numpy as jnp
from jax import lax
from jax.experimental import pallas as pl
from jax.experimental.pallas import tpu as pltpu
from jax.sharding import PartitionSpec as P

BLOCK = 128
ITERS = 5
GRID_BLK = 2
HIGHEST = lax.Precision.HIGHEST
MESH = pl.DeviceIdType.MESH


def block_terms(jac_part, weight_part, mask_part, predicted):
    scaled = (mask_part[:, None] * weight_part * predicted).astype(jnp.bfloat16)
    return lax.dot_general(
        jac_part, scaled, (((1,), (1,)), ((0,), (0,))), preferred_element_type=jnp.float32
    )


def forward_terms(jac_part, weight_part, mask_part, field_part):
    predicted = lax.dot_general(
        jac_part, field_part, (((2,), (1,)), ((0,), (0,))), preferred_element_type=jnp.float32
    )
    return block_terms(jac_part, weight_part, mask_part, predicted)


def exchange_per_step(jacobian, departures, obs_weights, column_count, grid_block, sqrt_cov):
    obs_count = lax.axis_size("obs")
    myself = lax.axis_index("obs")
    capacity, group_channels, layers = jacobian.shape
    block_count = capacity // BLOCK
    weight_cols = obs_weights.T
    depart_cols = departures.T
    observed = (jnp.arange(capacity, dtype=jnp.int32) < column_count[0]).astype(jnp.float32)
    every_id = lax.all_gather(grid_block, "obs", axis=0, tiled=True).reshape(obs_count, block_count)
    targets = jnp.arange(obs_count, dtype=jnp.int32)
    send_pick = (grid_block[None, :] // GRID_BLK == targets[:, None]).astype(jnp.float32)
    owned_here = every_id // GRID_BLK == myself
    places = every_id % GRID_BLK
    grid_index = jnp.arange(GRID_BLK, dtype=jnp.int32)
    take_pick = jnp.sum(
        ((places[None] == grid_index[:, None, None]) & owned_here[None]).astype(jnp.float32), axis=2
    )
    share_cols = BLOCK

    def local_terms(kernel_fn, inputs):
        return kernel_fn(jacobian, weight_cols, observed, inputs)

    def to_owners(terms):
        blocked = terms.reshape(block_count, BLOCK, layers)
        blocked = lax.psum(blocked, "chan")
        outgoing = jnp.dot(
            send_pick, blocked.reshape(block_count, -1), precision=lax.Precision.HIGHEST
        )
        incoming = lax.all_to_all(
            outgoing.reshape(obs_count, share_cols, layers),
            "obs",
            split_axis=0,
            concat_axis=0,
            tiled=True,
        )
        summed = jnp.dot(
            take_pick, incoming.reshape(obs_count, -1), precision=lax.Precision.HIGHEST
        )
        return summed.reshape(GRID_BLK, share_cols, layers)

    def spread(field):
        return jnp.dot(
            field.reshape(-1, layers), sqrt_cov, precision=lax.Precision.HIGHEST
        ).reshape(field.shape)

    def spread_back(field):
        flat = lax.dot_general(
            field.reshape(-1, layers),
            sqrt_cov,
            (((1,), (1,)), ((), ())),
            precision=lax.Precision.HIGHEST,
        )
        return flat.reshape(field.shape)

    def squared(values):
        partial_sum = jnp.sum(values * values)
        return lax.psum(partial_sum, "obs")

    residual = spread_back(to_owners(local_terms(block_terms, depart_cols)))
    control = jnp.zeros_like(residual)
    direction = residual
    norm_now = squared(residual)
    for iteration in range(ITERS):
        rounded = spread(direction).astype(jnp.bfloat16).reshape(GRID_BLK, -1)
        to_outgoing = jnp.dot(
            take_pick.T.astype(jnp.bfloat16), rounded, preferred_element_type=jnp.float32
        ).astype(jnp.bfloat16)
        to_incoming = lax.all_to_all(
            to_outgoing.reshape(obs_count, share_cols, layers),
            "obs",
            split_axis=0,
            concat_axis=0,
            tiled=True,
        )
        picked = jnp.dot(
            send_pick.T.astype(jnp.bfloat16),
            to_incoming.reshape(obs_count, -1),
            preferred_element_type=jnp.float32,
        )
        picked = picked.astype(jnp.bfloat16).reshape(block_count, share_cols, layers)
        fetched = picked.reshape(capacity, layers)
        image = direction + spread_back(to_owners(local_terms(forward_terms, fetched)))
        curvature_partial_sum = jnp.sum(direction * image)
        step_length = norm_now / lax.psum(curvature_partial_sum, "obs")
        control = control + step_length * direction
        residual = residual - step_length * image
        norm_next = squared(residual)
        direction = residual + norm_next / norm_now * direction
        norm_now = norm_next
    increment = spread(control)
    return (increment.reshape(-1, layers), residual.reshape(-1, layers))


LANES = 128
REST = 16


def cg_kernel(
    obs_count, chan_count, jac_ref, rest_ref, gram_ref, cov_ref, increment_ref, residual_ref,
    got_ref, got_rest_ref, wide_ref, turned_ref, weight_ref, parts_ref, back_ref,
    jac_send, jac_recv, rest_send, rest_recv, own_sem, sum_send, sum_recv, back_send, back_recv
):
    device_count = obs_count * chan_count
    me = lax.axis_index("obs") * chan_count + lax.axis_index("chan")
    layers = increment_ref.shape[1]
    block_count, share, channels = got_ref.shape[1:4]
    mine = block_count * share
    rows, padded, _ = turned_ref.shape
    lows = chan_count // 2
    grid_cols = GRID_BLK * obs_count * share
    piece = GRID_BLK * share

    def coords(target):
        return (target // chan_count, target % chan_count)

    barrier = pltpu.get_barrier_semaphore()

    def greet(offset, carry):
        pl.semaphore_signal(
            barrier, inc=1, device_id=coords((me + offset) % device_count), device_id_type=MESH
        )
        return carry

    lax.fori_loop(1, device_count, greet, 0)

    def own_part(block, target):
        return jac_ref.at[pl.ds(block * BLOCK + target * share, share), :, pl.ds(0, LANES)]

    own = [
        pltpu.make_async_copy(own_part(k, me), got_ref.at[me, k], own_sem.at[k])
        for k in range(block_count)
    ]
    own.append(pltpu.make_async_copy(rest_ref.at[me], got_rest_ref.at[me], own_sem.at[block_count]))
    for copy in own:
        copy.start()
    pl.semaphore_wait(barrier, device_count - 1)

    def send_columns(offset, carry):
        target = (me + offset) % device_count
        for k in range(block_count):
            pltpu.make_async_remote_copy(
                src_ref=own_part(k, target),
                dst_ref=got_ref.at[me, k],
                send_sem=jac_send,
                recv_sem=jac_recv,
                device_id=coords(target),
                device_id_type=MESH,
            ).start()
        pltpu.make_async_remote_copy(
            src_ref=rest_ref.at[target],
            dst_ref=got_rest_ref.at[me],
            send_sem=rest_send,
            recv_sem=rest_recv,
            device_id=coords(target),
            device_id_type=MESH,
        ).start()
        return carry

    lax.fori_loop(1, device_count, send_columns, 0)
    for copy in own:
        copy.wait()

    def wait_others(ref, sem):
        others = ref.at[pl.ds(0, device_count - 1)]
        pltpu.make_async_copy(others, others, sem).wait()

    wait_others(got_rest_ref, rest_recv)
    wait_others(got_rest_ref, rest_send)
    wait_others(got_ref, jac_recv)
    wait_others(got_ref, jac_send)

    def widen(source, carry):
        part = got_ref[source].astype(jnp.float32)
        wide_ref[pl.ds(source * mine * channels, mine * channels), :] = part.reshape(-1, LANES)
        return carry

    lax.fori_loop(0, device_count, widen, 0)

    def source_of(half, obs, low):
        return obs * chan_count + half * lows + low

    for low in range(lows):

        def turn(n, carry, low=low):
            picked = [
                wide_ref[pl.ds(source_of(half, obs, low) * mine * channels + n, mine, stride=channels), :]
                for half in range(2)
                for obs in range(obs_count)
            ]
            turned_ref[low * channels + n, 0:LANES, :] = jnp.concatenate(picked, axis=0).T
            return carry

        lax.fori_loop(0, channels, turn, 0, unroll=2)
        for half_rows in range(2):
            picked = [
                got_rest_ref[source_of(half, obs, low)].astype(jnp.float32)[
                    half_rows * mine : (half_rows + 1) * mine
                ]
                for half in range(2)
                for obs in range(obs_count)
            ]
            flipped = jnp.concatenate(picked, axis=0).T
            for n in range(channels // 2):
                turned_ref[low * channels + half_rows * (channels // 2) + n, LANES:padded, :] = (
                    flipped[n * REST : (n + 1) * REST]
                )

    def dot(a, b):
        return jnp.dot(a, b, precision=HIGHEST, preferred_element_type=jnp.float32)

    ids = turned_ref[0, layers + 3 : layers + 4, :].astype(jnp.int32)
    lane = lax.broadcasted_iota(jnp.int32, (grid_cols, LANES), 1)
    spot = lax.broadcasted_iota(jnp.int32, (grid_cols, LANES), 0)
    pick = (spot == ids * share + lane % share).astype(jnp.float32)

    def collect(terms):
        return lax.dot_general(
            terms, pick, (((1,), (1,)), ((), ())), precision=HIGHEST,
            preferred_element_type=jnp.float32,
        )

    def source_step(n, acc):
        kernel = turned_ref[n]
        weight_ref[pl.ds(n, 1), :] = kernel[layers : layers + 1] + kernel[layers + 1 : layers + 2]
        return acc + kernel * kernel[layers + 2 : layers + 3]

    zero = jnp.zeros((padded, LANES), jnp.float32)
    residual = collect(lax.fori_loop(0, rows, source_step, zero, unroll=4))

    control = direction = image = None
    norm_last = step_last = None
    for step in range(ITERS):
        spread = dot(gram_ref[...], residual)
        field = dot(spread, pick)

        def normal_step(n, acc):
            kernel = turned_ref[n]
            predicted = jnp.sum(kernel * field, axis=0, keepdims=True)
            return acc + kernel * (predicted * weight_ref[pl.ds(n, 1), :])

        terms = lax.fori_loop(0, rows, normal_step, zero, unroll=4)
        applied = residual + collect(terms)
        norm_part = jnp.sum(residual * spread, axis=0, keepdims=True)
        curve_part = jnp.sum(applied * spread, axis=0, keepdims=True)
        sub = lax.broadcasted_iota(jnp.int32, (8, grid_cols), 0)
        both = jnp.where(sub == 0, norm_part, jnp.where(sub == 1, curve_part, 0.0))
        if grid_cols < 128:
            both = jnp.concatenate([both, jnp.zeros((8, 128 - grid_cols), jnp.float32)], axis=1)
        parts_ref[step, me] = both

        def send_sum(offset, carry, step=step):
            pltpu.make_async_remote_copy(
                src_ref=parts_ref.at[step, me],
                dst_ref=parts_ref.at[step, me],
                send_sem=sum_send.at[step],
                recv_sem=sum_recv.at[step],
                device_id=coords((me + offset) % device_count),
                device_id_type=MESH,
            ).start()
            return carry

        lax.fori_loop(1, device_count, send_sum, 0)
        others = parts_ref.at[step, pl.ds(0, device_count - 1)]
        pltpu.make_async_copy(others, others, sum_recv.at[step]).wait()
        pltpu.make_async_copy(others, others, sum_send.at[step]).wait()
        total = jnp.sum(jnp.sum(parts_ref[step], axis=0), axis=1, keepdims=True)
        norm_now, curve = total[0:1], total[1:2]
        if step == 0:
            length = norm_now / curve
            direction, image = residual, applied
            control = length * direction
        else:
            ratio = norm_now / norm_last
            length = norm_now / (curve - ratio * norm_now / step_last)
            direction = residual + ratio * direction
            image = applied + ratio * image
            control = control + length * direction
        residual = residual - length * image
        norm_last, step_last = norm_now, length

    def flip_dot(a, b):
        return lax.dot_general(
            a, b, (((0,), (0,)), ((), ())), precision=HIGHEST, preferred_element_type=jnp.float32
        )

    outs = (flip_dot(control, gram_ref[...]), flip_dot(residual, cov_ref[...]))
    out_stage, landed = back_ref.at[0], back_ref.at[1]
    for which, value in enumerate(outs):
        for owner in range(obs_count):
            out_stage[owner * chan_count, which, :, :] = value[owner * piece : (owner + 1) * piece, :layers]
    landed[me] = out_stage[(me // chan_count) * chan_count]

    def send_back(offset, carry):
        target = (me + offset) % device_count
        pltpu.make_async_remote_copy(
            src_ref=out_stage.at[(target // chan_count) * chan_count],
            dst_ref=landed.at[me],
            send_sem=back_send,
            recv_sem=back_recv,
            device_id=coords(target),
            device_id_type=MESH,
        ).start()
        return carry

    lax.fori_loop(1, device_count, send_back, 0)
    others = landed.at[pl.ds(0, device_count - 1)]
    pltpu.make_async_copy(others, others, back_recv).wait()
    pltpu.make_async_copy(others, others, back_send).wait()
    for which, out_ref in enumerate((increment_ref, residual_ref)):
        for block in range(GRID_BLK):
            for source in range(device_count):
                first = block * BLOCK + source * share
                out_ref[first : first + share, :] = landed[
                    source, which, block * share : (block + 1) * share, :
                ]


def shared_columns(jacobian, departures, obs_weights, column_count, grid_block, sqrt_cov):
    obs_count, chan_count = lax.axis_size("obs"), lax.axis_size("chan")
    device_count = obs_count * chan_count
    capacity, channels, layers = jacobian.shape
    block_count = capacity // BLOCK
    share = BLOCK // device_count
    padded = LANES + REST
    rows = channels * chan_count // 2

    observed = (jnp.arange(capacity, dtype=jnp.int32) < column_count[0]).astype(jnp.float32)
    weight = observed[:, None] * obs_weights.T
    weight_high = weight.astype(jnp.bfloat16)
    weight_low = (weight - weight_high.astype(jnp.float32)).astype(jnp.bfloat16)
    source = (weight * departures.T).astype(jnp.bfloat16)
    ids = jnp.broadcast_to(jnp.repeat(grid_block, BLOCK)[:, None], weight.shape)
    extra = jnp.stack([weight_high, weight_low, source, ids.astype(jnp.bfloat16)], axis=2)
    rest = jnp.concatenate([jacobian[:, :, LANES:], extra], axis=2)
    rest = jnp.pad(rest, ((0, 0), (0, 0), (0, padded - layers - 4)))
    rest = rest.reshape(block_count, device_count, share, 2, channels // 2 * REST)
    rest = rest.transpose(1, 3, 0, 2, 4).reshape(
        device_count, 2 * block_count * share, channels // 2 * REST
    )
    fill = padded - layers
    gram = jnp.dot(sqrt_cov.T, sqrt_cov, precision=HIGHEST)
    gram = jnp.pad(gram, ((0, fill), (0, fill)))
    cov = jnp.pad(sqrt_cov.T, ((0, fill), (0, fill)))

    out = jax.ShapeDtypeStruct((GRID_BLK * BLOCK, layers), jnp.float32)
    vmem = pl.BlockSpec(memory_space=pltpu.VMEM)
    dma = pltpu.SemaphoreType.DMA
    return pl.pallas_call(
        functools.partial(cg_kernel, obs_count, chan_count),
        out_shape=(out, out),
        in_specs=[pl.BlockSpec(memory_space=pl.ANY)] + [vmem] * 3,
        out_specs=(vmem, vmem),
        scratch_shapes=[
            pltpu.VMEM((device_count, block_count, share, channels, LANES), jnp.bfloat16),
            pltpu.VMEM(rest.shape, jnp.bfloat16),
            pltpu.VMEM((device_count * block_count * share * channels, LANES), jnp.float32),
            pltpu.VMEM((rows, padded, LANES), jnp.float32),
            pltpu.VMEM((rows, LANES), jnp.float32),
            pltpu.VMEM((ITERS, device_count, 8, 128), jnp.float32),
            pltpu.VMEM((2, device_count, 2, GRID_BLK * share, layers), jnp.float32),
            dma, dma, dma, dma,
            dma((block_count + 1,)),
            dma((ITERS,)),
            dma((ITERS,)),
            dma, dma,
        ],
        compiler_params=pltpu.CompilerParams(
            collective_id=0, has_side_effects=True, vmem_limit_bytes=50 * 1024 * 1024
        ),
    )(jacobian, rest, gram, cov)


def solution(mesh):
    device_count = mesh.shape["obs"] * mesh.shape["chan"]

    def plan(jacobian, departures, obs_weights, column_count, grid_block, sqrt_cov):
        capacity, channels, layers = jacobian.shape
        mine = capacity // device_count
        fits = (
            BLOCK % device_count == 0
            and mine == 8
            and 2 * mesh.shape["obs"] * mine == LANES
            and mesh.shape["chan"] % 2 == 0
            and channels % 16 == 0
            and LANES < layers <= LANES + REST - 4
        )
        chosen = shared_columns if fits else exchange_per_step
        return chosen(jacobian, departures, obs_weights, column_count, grid_block, sqrt_cov)

    in_specs = (P("obs", "chan", None), P("chan", "obs"), P("chan", "obs"), P("obs"), P("obs"), P())
    out_specs = (P("obs", None), P("obs", None))
    return jax.shard_map(plan, mesh=mesh, in_specs=in_specs, out_specs=out_specs, check_vma=False)
```

```python
import functools
import jax
import jax.numpy as jnp
from jax import lax
from jax.experimental import pallas as pl
from jax.experimental.pallas import tpu as pltpu
from jax.sharding import PartitionSpec as P

BLOCK = 128
ITERS = 5
GRID_BLK = 2
HIGHEST = lax.Precision.HIGHEST
MESH = pl.DeviceIdType.MESH


def block_terms(jac_part, weight_part, mask_part, predicted):
    scaled = (mask_part[:, None] * weight_part * predicted).astype(jnp.bfloat16)
    return lax.dot_general(
        jac_part, scaled, (((1,), (1,)), ((0,), (0,))), preferred_element_type=jnp.float32
    )


def forward_terms(jac_part, weight_part, mask_part, field_part):
    predicted = lax.dot_general(
        jac_part, field_part, (((2,), (1,)), ((0,), (0,))), preferred_element_type=jnp.float32
    )
    return block_terms(jac_part, weight_part, mask_part, predicted)


def exchange_per_step(jacobian, departures, obs_weights, column_count, grid_block, sqrt_cov):
    obs_count = lax.axis_size("obs")
    myself = lax.axis_index("obs")
    capacity, group_channels, layers = jacobian.shape
    block_count = capacity // BLOCK
    weight_cols = obs_weights.T
    depart_cols = departures.T
    observed = (jnp.arange(capacity, dtype=jnp.int32) < column_count[0]).astype(jnp.float32)
    every_id = lax.all_gather(grid_block, "obs", axis=0, tiled=True).reshape(obs_count, block_count)
    targets = jnp.arange(obs_count, dtype=jnp.int32)
    send_pick = (grid_block[None, :] // GRID_BLK == targets[:, None]).astype(jnp.float32)
    owned_here = every_id // GRID_BLK == myself
    places = every_id % GRID_BLK
    grid_index = jnp.arange(GRID_BLK, dtype=jnp.int32)
    take_pick = jnp.sum(
        ((places[None] == grid_index[:, None, None]) & owned_here[None]).astype(jnp.float32), axis=2
    )
    share_cols = BLOCK

    def local_terms(kernel_fn, inputs):
        return kernel_fn(jacobian, weight_cols, observed, inputs)

    def to_owners(terms):
        blocked = terms.reshape(block_count, BLOCK, layers)
        blocked = lax.psum(blocked, "chan")
        outgoing = jnp.dot(
            send_pick, blocked.reshape(block_count, -1), precision=lax.Precision.HIGHEST
        )
        incoming = lax.all_to_all(
            outgoing.reshape(obs_count, share_cols, layers),
            "obs",
            split_axis=0,
            concat_axis=0,
            tiled=True,
        )
        summed = jnp.dot(
            take_pick, incoming.reshape(obs_count, -1), precision=lax.Precision.HIGHEST
        )
        return summed.reshape(GRID_BLK, share_cols, layers)

    def spread(field):
        return jnp.dot(
            field.reshape(-1, layers), sqrt_cov, precision=lax.Precision.HIGHEST
        ).reshape(field.shape)

    def spread_back(field):
        flat = lax.dot_general(
            field.reshape(-1, layers),
            sqrt_cov,
            (((1,), (1,)), ((), ())),
            precision=lax.Precision.HIGHEST,
        )
        return flat.reshape(field.shape)

    def squared(values):
        partial_sum = jnp.sum(values * values)
        return lax.psum(partial_sum, "obs")

    residual = spread_back(to_owners(local_terms(block_terms, depart_cols)))
    control = jnp.zeros_like(residual)
    direction = residual
    norm_now = squared(residual)
    for iteration in range(ITERS):
        rounded = spread(direction).astype(jnp.bfloat16).reshape(GRID_BLK, -1)
        to_outgoing = jnp.dot(
            take_pick.T.astype(jnp.bfloat16), rounded, preferred_element_type=jnp.float32
        ).astype(jnp.bfloat16)
        to_incoming = lax.all_to_all(
            to_outgoing.reshape(obs_count, share_cols, layers),
            "obs",
            split_axis=0,
            concat_axis=0,
            tiled=True,
        )
        picked = jnp.dot(
            send_pick.T.astype(jnp.bfloat16),
            to_incoming.reshape(obs_count, -1),
            preferred_element_type=jnp.float32,
        )
        picked = picked.astype(jnp.bfloat16).reshape(block_count, share_cols, layers)
        fetched = picked.reshape(capacity, layers)
        image = direction + spread_back(to_owners(local_terms(forward_terms, fetched)))
        curvature_partial_sum = jnp.sum(direction * image)
        step_length = norm_now / lax.psum(curvature_partial_sum, "obs")
        control = control + step_length * direction
        residual = residual - step_length * image
        norm_next = squared(residual)
        direction = residual + norm_next / norm_now * direction
        norm_now = norm_next
    increment = spread(control)
    return (increment.reshape(-1, layers), residual.reshape(-1, layers))


LANES = 128
REST = 16


def cg_kernel(
    obs_count, chan_count, jac_ref, rest_ref, gram_ref, cov_ref, increment_ref, residual_ref,
    got_ref, put_rest_ref, got_rest_ref, wide_ref, turned_ref, weight_ref, parts_ref, back_ref,
    jac_send, jac_recv, rest_send, rest_recv, own_sem, sum_send, sum_recv, back_send, back_recv
):
    device_count = obs_count * chan_count
    me = lax.axis_index("obs") * chan_count + lax.axis_index("chan")
    layers = increment_ref.shape[1]
    _, _, block_count, share, half_channels, _ = got_ref.shape
    channels = 2 * half_channels
    mine = block_count * share
    rows, padded, _ = turned_ref.shape
    lows = chan_count // 2
    grid_cols = GRID_BLK * obs_count * share
    piece = GRID_BLK * share

    def coords(target):
        return (target // chan_count, target % chan_count)

    barrier = pltpu.get_barrier_semaphore()

    def greet(offset, carry):
        pl.semaphore_signal(
            barrier, inc=1, device_id=coords((me + offset) % device_count), device_id_type=MESH
        )
        return carry

    lax.fori_loop(1, device_count, greet, 0)

    def own_part(part, block, target):
        return jac_ref.at[
            pl.ds(block * BLOCK + target * share, share), pl.ds(part * half_channels, half_channels), :
        ]

    own = [
        pltpu.make_async_copy(
            own_part(part, k, me), got_ref.at[part, me, k], own_sem.at[part * block_count + k]
        )
        for part in range(2)
        for k in range(block_count)
    ]
    for copy in own:
        copy.start()
    pl.semaphore_wait(barrier, device_count - 1)

    def send_columns(part):
        def send(offset, carry):
            target = (me + offset) % device_count
            for k in range(block_count):
                pltpu.make_async_remote_copy(
                    src_ref=own_part(part, k, target),
                    dst_ref=got_ref.at[part, me, k],
                    send_sem=jac_send.at[part],
                    recv_sem=jac_recv.at[part],
                    device_id=coords(target),
                    device_id_type=MESH,
                ).start()
            return carry

        lax.fori_loop(1, device_count, send, 0)

    def send_rest(offset, carry):
        target = (me + offset) % device_count
        pltpu.make_async_remote_copy(
            src_ref=put_rest_ref.at[target],
            dst_ref=got_rest_ref.at[me],
            send_sem=rest_send,
            recv_sem=rest_recv,
            device_id=coords(target),
            device_id_type=MESH,
        ).start()
        return carry

    send_columns(0)
    columns = block_count * BLOCK
    row = lax.broadcasted_iota(jnp.int32, (columns, columns), 0)
    column = lax.broadcasted_iota(jnp.int32, (columns, columns), 1)
    wanted = (row % mine) // share * BLOCK + row // mine * share + row % share
    order = jnp.where(column == wanted, 1.0, 0.0).astype(jnp.bfloat16)
    ordered = lax.dot_general(
        order, rest_ref[...], (((1,), (1,)), ((), ())), preferred_element_type=jnp.float32
    )
    width = half_channels * REST
    for part in range(2):
        strip = ordered[:, part * width : (part + 1) * width].astype(jnp.bfloat16)
        put_rest_ref[:, part * mine : (part + 1) * mine, :] = strip.reshape(device_count, mine, width)
    got_rest_ref[me] = put_rest_ref[me]
    lax.fori_loop(1, device_count, send_rest, 0)
    send_columns(1)
    for copy in own:
        copy.wait()

    def wait_others(ref, sem):
        others = ref.at[pl.ds(0, device_count - 1)]
        pltpu.make_async_copy(others, others, sem).wait()

    wait_others(got_rest_ref, rest_recv)
    wait_others(got_rest_ref, rest_send)

    def widen(part):
        def step(source, carry):
            block = got_ref[part, source].astype(jnp.float32).reshape(-1, LANES)
            wide_ref[pl.ds(source * mine * half_channels, mine * half_channels), :] = block
            return carry

        lax.fori_loop(0, device_count, step, 0)

    def source_of(half, obs, low):
        return obs * chan_count + half * lows + low

    def turn_half(part, low):
        first = low * channels + part * half_channels

        def turn(n, carry):
            picked = [
                wide_ref[
                    pl.ds(source_of(half, obs, low) * mine * half_channels + n, mine, stride=half_channels), :
                ]
                for half in range(2)
                for obs in range(obs_count)
            ]
            turned_ref[first + n, 0:LANES, :] = jnp.concatenate(picked, axis=0).T
            return carry

        lax.fori_loop(0, half_channels, turn, 0, unroll=2)
        picked = [
            got_rest_ref[source_of(half, obs, low)].astype(jnp.float32)[part * mine : (part + 1) * mine]
            for half in range(2)
            for obs in range(obs_count)
        ]
        flipped = jnp.concatenate(picked, axis=0).T
        for n in range(half_channels):
            turned_ref[first + n, LANES:padded, :] = flipped[n * REST : (n + 1) * REST]

    for part in range(2):
        others = got_ref.at[part, pl.ds(0, device_count - 1)]
        pltpu.make_async_copy(others, others, jac_recv.at[part]).wait()
        pltpu.make_async_copy(others, others, jac_send.at[part]).wait()
        widen(part)
        for low in range(lows):
            turn_half(part, low)

    def dot(a, b):
        return jnp.dot(a, b, precision=HIGHEST, preferred_element_type=jnp.float32)

    ids = turned_ref[0, layers + 3 : layers + 4, :].astype(jnp.int32)
    lane = lax.broadcasted_iota(jnp.int32, (grid_cols, LANES), 1)
    spot = lax.broadcasted_iota(jnp.int32, (grid_cols, LANES), 0)
    pick = (spot == ids * share + lane % share).astype(jnp.float32)

    def times(a, b, b_dim):
        total = None
        for _ in range(3):
            part = a.astype(jnp.bfloat16)
            a = a - part.astype(jnp.float32)
            product = lax.dot_general(
                part, b, (((1,), (b_dim,)), ((), ())), preferred_element_type=jnp.float32
            )
            total = product if total is None else total + product
        return total

    picked_bf16 = pick.astype(jnp.bfloat16)
    shared = lax.dot_general(
        picked_bf16, picked_bf16, (((0,), (0,)), ((), ())), preferred_element_type=jnp.float32
    )
    copies = jnp.sum(shared, axis=0, keepdims=True)
    shared = shared.astype(jnp.bfloat16)

    def collect(terms):
        return times(terms, shared, 0)

    def source_step(n, acc):
        kernel = turned_ref[n]
        weight_ref[pl.ds(n, 1), :] = kernel[layers : layers + 1] + kernel[layers + 1 : layers + 2]
        return acc + kernel * kernel[layers + 2 : layers + 3]

    zero = jnp.zeros((padded, LANES), jnp.float32)
    residual = collect(lax.fori_loop(0, rows, source_step, zero, unroll=4))

    def normal(field, spread):
        def normal_step(n, acc):
            kernel = turned_ref[n]
            predicted = jnp.sum(kernel * spread, axis=0, keepdims=True)
            return acc + kernel * (predicted * weight_ref[pl.ds(n, 1), :])

        return field + collect(lax.fori_loop(0, rows, normal_step, zero, unroll=4))

    share_of = 1.0 / copies
    spread = dot(gram_ref[...], residual)
    applied = normal(residual, spread)
    control = direction = image = spread_image = image_applied = None
    norm_last = step_last = None
    for step in range(ITERS):
        norm_part = jnp.sum(residual * spread, axis=0, keepdims=True) * share_of
        curve_part = jnp.sum(applied * spread, axis=0, keepdims=True) * share_of
        sub = lax.broadcasted_iota(jnp.int32, (8, LANES), 0)
        parts_ref[step, me] = jnp.where(sub == 0, norm_part, jnp.where(sub == 1, curve_part, 0.0))

        def send_sum(offset, carry, step=step):
            pltpu.make_async_remote_copy(
                src_ref=parts_ref.at[step, me],
                dst_ref=parts_ref.at[step, me],
                send_sem=sum_send.at[step],
                recv_sem=sum_recv.at[step],
                device_id=coords((me + offset) % device_count),
                device_id_type=MESH,
            ).start()
            return carry

        lax.fori_loop(1, device_count, send_sum, 0)
        last = step == ITERS - 1
        if not last:
            next_spread = dot(gram_ref[...], applied)
            next_applied = normal(applied, next_spread)
        others = parts_ref.at[step, pl.ds(0, device_count - 1)]
        pltpu.make_async_copy(others, others, sum_recv.at[step]).wait()
        pltpu.make_async_copy(others, others, sum_send.at[step]).wait()
        total = jnp.sum(jnp.sum(parts_ref[step], axis=0), axis=1, keepdims=True)
        norm_now, curve = total[0:1], total[1:2]
        if step == 0:
            length = norm_now / curve
            direction, image = residual, applied
            spread_image, image_applied = next_spread, next_applied
            control = length * direction
        else:
            ratio = norm_now / norm_last
            length = norm_now / (curve - ratio * norm_now / step_last)
            direction = residual + ratio * direction
            image = applied + ratio * image
            if not last:
                spread_image = next_spread + ratio * spread_image
                image_applied = next_applied + ratio * image_applied
            control = control + length * direction
        residual = residual - length * image
        if not last:
            spread = spread - length * spread_image
            applied = applied - length * image_applied
        norm_last, step_last = norm_now, length
    control = times(control * share_of, picked_bf16, 1)
    residual = times(residual * share_of, picked_bf16, 1)

    def flip_dot(a, b):
        return lax.dot_general(
            a, b, (((0,), (0,)), ((), ())), precision=HIGHEST, preferred_element_type=jnp.float32
        )

    outs = (flip_dot(control, gram_ref[...]), flip_dot(residual, cov_ref[...]))
    out_stage, landed = back_ref.at[0], back_ref.at[1]
    for which, value in enumerate(outs):
        for owner in range(obs_count):
            out_stage[owner * chan_count, which, :, :] = value[owner * piece : (owner + 1) * piece, :layers]
    landed[me] = out_stage[(me // chan_count) * chan_count]

    def send_back(offset, carry):
        target = (me + offset) % device_count
        pltpu.make_async_remote_copy(
            src_ref=out_stage.at[(target // chan_count) * chan_count],
            dst_ref=landed.at[me],
            send_sem=back_send,
            recv_sem=back_recv,
            device_id=coords(target),
            device_id_type=MESH,
        ).start()
        return carry

    lax.fori_loop(1, device_count, send_back, 0)
    others = landed.at[pl.ds(0, device_count - 1)]
    pltpu.make_async_copy(others, others, back_recv).wait()
    pltpu.make_async_copy(others, others, back_send).wait()
    for which, out_ref in enumerate((increment_ref, residual_ref)):
        for block in range(GRID_BLK):
            for source in range(device_count):
                first = block * BLOCK + source * share
                out_ref[first : first + share, :] = landed[
                    source, which, block * share : (block + 1) * share, :
                ]


def shared_columns(jacobian, departures, obs_weights, column_count, grid_block, sqrt_cov):
    obs_count, chan_count = lax.axis_size("obs"), lax.axis_size("chan")
    device_count = obs_count * chan_count
    capacity, channels, layers = jacobian.shape
    block_count = capacity // BLOCK
    share = BLOCK // device_count
    padded = LANES + REST
    rows = channels * chan_count // 2

    observed = (jnp.arange(capacity, dtype=jnp.int32) < column_count[0]).astype(jnp.float32)
    weight = observed[None, :] * obs_weights
    weight_high = weight.astype(jnp.bfloat16)
    weight_low = (weight - weight_high.astype(jnp.float32)).astype(jnp.bfloat16)
    source = (weight * departures).astype(jnp.bfloat16)
    ids = jnp.broadcast_to(jnp.repeat(grid_block, BLOCK)[None, :], weight.shape)
    extra = jnp.stack([weight_high, weight_low, source, ids.astype(jnp.bfloat16)], axis=1)
    rest = jnp.concatenate([jacobian[:, :, LANES:].transpose(1, 2, 0), extra], axis=1)
    rest = jnp.pad(rest, ((0, 0), (0, padded - layers - 4), (0, 0)))
    rest = rest.reshape(channels * REST, capacity)
    rest_shape = (device_count, 2 * block_count * share, channels // 2 * REST)
    fill = padded - layers
    gram = jnp.dot(sqrt_cov.T, sqrt_cov, precision=HIGHEST)
    gram = jnp.pad(gram, ((0, fill), (0, fill)))
    cov = jnp.pad(sqrt_cov.T, ((0, fill), (0, fill)))

    out = jax.ShapeDtypeStruct((GRID_BLK * BLOCK, layers), jnp.float32)
    vmem = pl.BlockSpec(memory_space=pltpu.VMEM)
    dma = pltpu.SemaphoreType.DMA
    return pl.pallas_call(
        functools.partial(cg_kernel, obs_count, chan_count),
        out_shape=(out, out),
        in_specs=[pl.BlockSpec(memory_space=pl.ANY)] + [vmem] * 3,
        out_specs=(vmem, vmem),
        scratch_shapes=[
            pltpu.VMEM((2, device_count, block_count, share, channels // 2, LANES), jnp.bfloat16),
            pltpu.VMEM(rest_shape, jnp.bfloat16),
            pltpu.VMEM(rest_shape, jnp.bfloat16),
            pltpu.VMEM((device_count * block_count * share * channels // 2, LANES), jnp.float32),
            pltpu.VMEM((rows, padded, LANES), jnp.float32),
            pltpu.VMEM((rows, LANES), jnp.float32),
            pltpu.VMEM((ITERS, device_count, 8, 128), jnp.float32),
            pltpu.VMEM((2, device_count, 2, GRID_BLK * share, layers), jnp.float32),
            dma((2,)), dma((2,)), dma, dma,
            dma((2 * block_count,)),
            dma((ITERS,)),
            dma((ITERS,)),
            dma, dma,
        ],
        compiler_params=pltpu.CompilerParams(
            collective_id=0, has_side_effects=True, vmem_limit_bytes=50 * 1024 * 1024
        ),
    )(jacobian[:, :, :LANES], rest, gram, cov)


def solution(mesh):
    device_count = mesh.shape["obs"] * mesh.shape["chan"]

    def plan(jacobian, departures, obs_weights, column_count, grid_block, sqrt_cov):
        capacity, channels, layers = jacobian.shape
        mine = capacity // device_count
        fits = (
            BLOCK % device_count == 0
            and mine == 8
            and 2 * mesh.shape["obs"] * mine == LANES
            and mesh.shape["chan"] % 2 == 0
            and channels % 32 == 0
            and LANES < layers <= LANES + REST - 4
        )
        chosen = shared_columns if fits else exchange_per_step
        return chosen(jacobian, departures, obs_weights, column_count, grid_block, sqrt_cov)

    in_specs = (P("obs", "chan", None), P("chan", "obs"), P("chan", "obs"), P("obs"), P("obs"), P())
    out_specs = (P("obs", None), P("obs", None))
    return jax.shard_map(plan, mesh=mesh, in_specs=in_specs, out_specs=out_specs, check_vma=False)
```

```python
import functools
import jax
import jax.numpy as jnp
from jax import lax
from jax.experimental import pallas as pl
from jax.experimental.pallas import tpu as pltpu
from jax.sharding import PartitionSpec as P

BLOCK = 128
ITERS = 5
GRID_BLK = 2
HIGHEST = lax.Precision.HIGHEST
MESH = pl.DeviceIdType.MESH


def block_terms(jac_part, weight_part, mask_part, predicted):
    scaled = (mask_part[:, None] * weight_part * predicted).astype(jnp.bfloat16)
    return lax.dot_general(
        jac_part, scaled, (((1,), (1,)), ((0,), (0,))), preferred_element_type=jnp.float32
    )


def forward_terms(jac_part, weight_part, mask_part, field_part):
    predicted = lax.dot_general(
        jac_part, field_part, (((2,), (1,)), ((0,), (0,))), preferred_element_type=jnp.float32
    )
    return block_terms(jac_part, weight_part, mask_part, predicted)


def exchange_per_step(jacobian, departures, obs_weights, column_count, grid_block, sqrt_cov):
    obs_count = lax.axis_size("obs")
    myself = lax.axis_index("obs")
    capacity, group_channels, layers = jacobian.shape
    block_count = capacity // BLOCK
    weight_cols = obs_weights.T
    depart_cols = departures.T
    observed = (jnp.arange(capacity, dtype=jnp.int32) < column_count[0]).astype(jnp.float32)
    every_id = lax.all_gather(grid_block, "obs", axis=0, tiled=True).reshape(obs_count, block_count)
    targets = jnp.arange(obs_count, dtype=jnp.int32)
    send_pick = (grid_block[None, :] // GRID_BLK == targets[:, None]).astype(jnp.float32)
    owned_here = every_id // GRID_BLK == myself
    places = every_id % GRID_BLK
    grid_index = jnp.arange(GRID_BLK, dtype=jnp.int32)
    take_pick = jnp.sum(
        ((places[None] == grid_index[:, None, None]) & owned_here[None]).astype(jnp.float32), axis=2
    )
    share_cols = BLOCK

    def local_terms(kernel_fn, inputs):
        return kernel_fn(jacobian, weight_cols, observed, inputs)

    def to_owners(terms):
        blocked = terms.reshape(block_count, BLOCK, layers)
        blocked = lax.psum(blocked, "chan")
        outgoing = jnp.dot(
            send_pick, blocked.reshape(block_count, -1), precision=lax.Precision.HIGHEST
        )
        incoming = lax.all_to_all(
            outgoing.reshape(obs_count, share_cols, layers),
            "obs",
            split_axis=0,
            concat_axis=0,
            tiled=True,
        )
        summed = jnp.dot(
            take_pick, incoming.reshape(obs_count, -1), precision=lax.Precision.HIGHEST
        )
        return summed.reshape(GRID_BLK, share_cols, layers)

    def spread(field):
        return jnp.dot(
            field.reshape(-1, layers), sqrt_cov, precision=lax.Precision.HIGHEST
        ).reshape(field.shape)

    def spread_back(field):
        flat = lax.dot_general(
            field.reshape(-1, layers),
            sqrt_cov,
            (((1,), (1,)), ((), ())),
            precision=lax.Precision.HIGHEST,
        )
        return flat.reshape(field.shape)

    def squared(values):
        partial_sum = jnp.sum(values * values)
        return lax.psum(partial_sum, "obs")

    residual = spread_back(to_owners(local_terms(block_terms, depart_cols)))
    control = jnp.zeros_like(residual)
    direction = residual
    norm_now = squared(residual)
    for iteration in range(ITERS):
        rounded = spread(direction).astype(jnp.bfloat16).reshape(GRID_BLK, -1)
        to_outgoing = jnp.dot(
            take_pick.T.astype(jnp.bfloat16), rounded, preferred_element_type=jnp.float32
        ).astype(jnp.bfloat16)
        to_incoming = lax.all_to_all(
            to_outgoing.reshape(obs_count, share_cols, layers),
            "obs",
            split_axis=0,
            concat_axis=0,
            tiled=True,
        )
        picked = jnp.dot(
            send_pick.T.astype(jnp.bfloat16),
            to_incoming.reshape(obs_count, -1),
            preferred_element_type=jnp.float32,
        )
        picked = picked.astype(jnp.bfloat16).reshape(block_count, share_cols, layers)
        fetched = picked.reshape(capacity, layers)
        image = direction + spread_back(to_owners(local_terms(forward_terms, fetched)))
        curvature_partial_sum = jnp.sum(direction * image)
        step_length = norm_now / lax.psum(curvature_partial_sum, "obs")
        control = control + step_length * direction
        residual = residual - step_length * image
        norm_next = squared(residual)
        direction = residual + norm_next / norm_now * direction
        norm_now = norm_next
    increment = spread(control)
    return (increment.reshape(-1, layers), residual.reshape(-1, layers))


LANES = 128
REST = 16
STRIDE = 11


def cg_kernel(
    obs_count, chan_count, jac_ref, rest_ref, gram_ref, cov_ref, increment_ref, residual_ref,
    got_ref, put_rest_ref, got_rest_ref, wide_ref, turned_ref, weight_ref, parts_ref, back_ref,
    jac_send, jac_recv, rest_send, rest_recv, own_sem, sum_send, sum_recv, back_send, back_recv
):
    device_count = obs_count * chan_count
    me = lax.axis_index("obs") * chan_count + lax.axis_index("chan")
    layers = increment_ref.shape[1]
    _, _, block_count, share, half_channels, _ = got_ref.shape
    channels = 2 * half_channels
    mine = block_count * share
    rows, padded, _ = turned_ref.shape
    lows = chan_count // 2
    grid_cols = GRID_BLK * obs_count * share
    piece = GRID_BLK * share

    def coords(target):
        return (target // chan_count, target % chan_count)

    barrier = pltpu.get_barrier_semaphore()

    def greet(offset, carry):
        pl.semaphore_signal(
            barrier, inc=1, device_id=coords((me + offset) % device_count), device_id_type=MESH
        )
        return carry

    lax.fori_loop(1, device_count, greet, 0)

    def own_part(part, block, target):
        return jac_ref.at[
            pl.ds(block * BLOCK + target * share, share), pl.ds(part * half_channels, half_channels), pl.ds(0, LANES)
        ]

    own = [
        pltpu.make_async_copy(
            own_part(part, k, me), got_ref.at[part, me, k], own_sem.at[part * block_count + k]
        )
        for part in range(2)
        for k in range(block_count)
    ]
    for copy in own:
        copy.start()
    pl.semaphore_wait(barrier, device_count - 1)

    def send_columns(part):
        def send(offset, carry):
            target = (me + offset * STRIDE) % device_count
            for k in range(block_count):
                pltpu.make_async_remote_copy(
                    src_ref=own_part(part, k, target),
                    dst_ref=got_ref.at[part, me, k],
                    send_sem=jac_send.at[part],
                    recv_sem=jac_recv.at[part],
                    device_id=coords(target),
                    device_id_type=MESH,
                ).start()
            return carry

        lax.fori_loop(1, device_count, send, 0)

    def send_rest(offset, carry):
        target = (me + offset * STRIDE) % device_count
        pltpu.make_async_remote_copy(
            src_ref=put_rest_ref.at[target],
            dst_ref=got_rest_ref.at[me],
            send_sem=rest_send,
            recv_sem=rest_recv,
            device_id=coords(target),
            device_id_type=MESH,
        ).start()
        return carry

    send_columns(0)
    columns = block_count * BLOCK
    row = lax.broadcasted_iota(jnp.int32, (columns, columns), 0)
    column = lax.broadcasted_iota(jnp.int32, (columns, columns), 1)
    wanted = (row % mine) // share * BLOCK + row // mine * share + row % share
    order = jnp.where(column == wanted, 1.0, 0.0).astype(jnp.bfloat16)
    ordered = lax.dot_general(
        order, rest_ref[...], (((1,), (1,)), ((), ())), preferred_element_type=jnp.float32
    )
    width = half_channels * REST
    for part in range(2):
        strip = ordered[:, part * width : (part + 1) * width].astype(jnp.bfloat16)
        put_rest_ref[:, part * mine : (part + 1) * mine, :] = strip.reshape(device_count, mine, width)
    got_rest_ref[me] = put_rest_ref[me]
    lax.fori_loop(1, device_count, send_rest, 0)
    send_columns(1)
    for copy in own:
        copy.wait()

    def wait_others(ref, sem):
        others = ref.at[pl.ds(0, device_count - 1)]
        pltpu.make_async_copy(others, others, sem).wait()

    wait_others(got_rest_ref, rest_recv)
    wait_others(got_rest_ref, rest_send)

    def widen(part):
        def step(source, carry):
            block = got_ref[part, source].astype(jnp.float32).reshape(-1, LANES)
            wide_ref[pl.ds(source * mine * half_channels, mine * half_channels), :] = block
            return carry

        lax.fori_loop(0, device_count, step, 0)

    def source_of(half, obs, low):
        return obs * chan_count + half * lows + low

    def turn_half(part, low):
        first = low * channels + part * half_channels

        def turn(n, carry):
            picked = [
                wide_ref[
                    pl.ds(source_of(half, obs, low) * mine * half_channels + n, mine, stride=half_channels), :
                ]
                for half in range(2)
                for obs in range(obs_count)
            ]
            turned_ref[first + n, 0:LANES, :] = jnp.concatenate(picked, axis=0).T
            return carry

        lax.fori_loop(0, half_channels, turn, 0, unroll=2)
        picked = [
            got_rest_ref[source_of(half, obs, low)].astype(jnp.float32)[part * mine : (part + 1) * mine]
            for half in range(2)
            for obs in range(obs_count)
        ]
        flipped = jnp.concatenate(picked, axis=0).T
        for n in range(half_channels):
            turned_ref[first + n, LANES:padded, :] = flipped[n * REST : (n + 1) * REST]

    for part in range(2):
        others = got_ref.at[part, pl.ds(0, device_count - 1)]
        pltpu.make_async_copy(others, others, jac_recv.at[part]).wait()
        pltpu.make_async_copy(others, others, jac_send.at[part]).wait()
        widen(part)
        for low in range(lows):
            turn_half(part, low)

    def dot(a, b):
        return jnp.dot(a, b, precision=HIGHEST, preferred_element_type=jnp.float32)

    ids = turned_ref[0, layers + 3 : layers + 4, :].astype(jnp.int32)
    lane = lax.broadcasted_iota(jnp.int32, (grid_cols, LANES), 1)
    spot = lax.broadcasted_iota(jnp.int32, (grid_cols, LANES), 0)
    pick = (spot == ids * share + lane % share).astype(jnp.float32)

    def times(a, b, b_dim):
        total = None
        for _ in range(3):
            part = a.astype(jnp.bfloat16)
            a = a - part.astype(jnp.float32)
            product = lax.dot_general(
                part, b, (((1,), (b_dim,)), ((), ())), preferred_element_type=jnp.float32
            )
            total = product if total is None else total + product
        return total

    picked_bf16 = pick.astype(jnp.bfloat16)
    shared = lax.dot_general(
        picked_bf16, picked_bf16, (((0,), (0,)), ((), ())), preferred_element_type=jnp.float32
    )
    copies = jnp.sum(shared, axis=0, keepdims=True)
    shared = shared.astype(jnp.bfloat16)

    def collect(terms):
        return times(terms, shared, 0)

    def source_step(n, acc):
        kernel = turned_ref[n]
        weight_ref[pl.ds(n, 1), :] = kernel[layers : layers + 1] + kernel[layers + 1 : layers + 2]
        return acc + kernel * kernel[layers + 2 : layers + 3]

    zero = jnp.zeros((padded, LANES), jnp.float32)
    residual = collect(lax.fori_loop(0, rows, source_step, zero, unroll=4))

    def normal(field, spread):
        def normal_step(n, acc):
            kernel = turned_ref[n]
            predicted = jnp.sum(kernel * spread, axis=0, keepdims=True)
            return acc + kernel * (predicted * weight_ref[pl.ds(n, 1), :])

        return field + collect(lax.fori_loop(0, rows, normal_step, zero, unroll=4))

    share_of = 1.0 / copies
    spread = dot(gram_ref[...], residual)
    applied = normal(residual, spread)
    control = direction = image = spread_image = image_applied = None
    norm_last = step_last = None
    for step in range(ITERS):
        norm_part = jnp.sum(residual * spread, axis=0, keepdims=True) * share_of
        curve_part = jnp.sum(applied * spread, axis=0, keepdims=True) * share_of
        norm_part = jnp.sum(norm_part, axis=1, keepdims=True)
        curve_part = jnp.sum(curve_part, axis=1, keepdims=True)
        place = lax.broadcasted_iota(jnp.int32, (1, LANES), 1)
        parts_ref[step, me] = jnp.where(place == 0, norm_part, jnp.where(place == 1, curve_part, 0.0))

        def send_sum(offset, carry, step=step):
            pltpu.make_async_remote_copy(
                src_ref=parts_ref.at[step, me],
                dst_ref=parts_ref.at[step, me],
                send_sem=sum_send.at[step],
                recv_sem=sum_recv.at[step],
                device_id=coords((me + offset) % device_count),
                device_id_type=MESH,
            ).start()
            return carry

        lax.fori_loop(1, device_count, send_sum, 0)
        last = step == ITERS - 1
        if not last:
            next_spread = dot(gram_ref[...], applied)
            next_applied = normal(applied, next_spread)
        others = parts_ref.at[step, pl.ds(0, device_count - 1)]
        pltpu.make_async_copy(others, others, sum_recv.at[step]).wait()
        pltpu.make_async_copy(others, others, sum_send.at[step]).wait()
        total = jnp.sum(parts_ref[step], axis=0)
        norm_now = jnp.sum(jnp.where(place == 0, total, 0.0), axis=1, keepdims=True)
        curve = jnp.sum(jnp.where(place == 1, total, 0.0), axis=1, keepdims=True)
        if step == 0:
            length = norm_now / curve
            direction, image = residual, applied
            spread_image, image_applied = next_spread, next_applied
            control = length * direction
        else:
            ratio = norm_now / norm_last
            length = norm_now / (curve - ratio * norm_now / step_last)
            direction = residual + ratio * direction
            image = applied + ratio * image
            if not last:
                spread_image = next_spread + ratio * spread_image
                image_applied = next_applied + ratio * image_applied
            control = control + length * direction
        residual = residual - length * image
        if not last:
            spread = spread - length * spread_image
            applied = applied - length * image_applied
        norm_last, step_last = norm_now, length
    control = times(control * share_of, picked_bf16, 1)
    residual = times(residual * share_of, picked_bf16, 1)

    def flip_dot(a, b):
        return lax.dot_general(
            a, b, (((0,), (0,)), ((), ())), precision=HIGHEST, preferred_element_type=jnp.float32
        )

    outs = (flip_dot(control, gram_ref[...]), flip_dot(residual, cov_ref[...]))
    out_stage, landed = back_ref.at[0], back_ref.at[1]
    for owner in range(obs_count):
        pieces = [value[owner * piece : (owner + 1) * piece, :layers] for value in outs]
        out_stage[owner * chan_count, :, :] = jnp.concatenate(pieces, axis=0).astype(jnp.bfloat16)
    landed[me] = out_stage[(me // chan_count) * chan_count]

    def send_back(offset, carry):
        target = (me + offset) % device_count
        pltpu.make_async_remote_copy(
            src_ref=out_stage.at[(target // chan_count) * chan_count],
            dst_ref=landed.at[me],
            send_sem=back_send,
            recv_sem=back_recv,
            device_id=coords(target),
            device_id_type=MESH,
        ).start()
        return carry

    lax.fori_loop(1, device_count, send_back, 0)
    others = landed.at[pl.ds(0, device_count - 1)]
    pltpu.make_async_copy(others, others, back_recv).wait()
    pltpu.make_async_copy(others, others, back_send).wait()
    for source in range(device_count):
        block_rows = landed[source].astype(jnp.float32)
        for which, out_ref in enumerate((increment_ref, residual_ref)):
            for block in range(GRID_BLK):
                first = block * BLOCK + source * share
                taken = which * piece + block * share
                out_ref[first : first + share, :] = block_rows[taken : taken + share]


def shared_columns(jacobian, departures, obs_weights, column_count, grid_block, sqrt_cov):
    obs_count, chan_count = lax.axis_size("obs"), lax.axis_size("chan")
    device_count = obs_count * chan_count
    capacity, channels, layers = jacobian.shape
    block_count = capacity // BLOCK
    share = BLOCK // device_count
    padded = LANES + REST
    rows = channels * chan_count // 2

    observed = (jnp.arange(capacity, dtype=jnp.int32) < column_count[0]).astype(jnp.float32)
    weight = observed[None, :] * obs_weights
    weight_high = weight.astype(jnp.bfloat16)
    weight_low = (weight - weight_high.astype(jnp.float32)).astype(jnp.bfloat16)
    source = (weight * departures).astype(jnp.bfloat16)
    ids = jnp.broadcast_to(jnp.repeat(grid_block, BLOCK)[None, :], weight.shape)
    extra = jnp.stack([weight_high, weight_low, source, ids.astype(jnp.bfloat16)], axis=1)
    rest = jnp.concatenate([jacobian[:, :, LANES:].transpose(1, 2, 0), extra], axis=1)
    rest = jnp.pad(rest, ((0, 0), (0, padded - layers - 4), (0, 0)))
    rest = rest.reshape(channels * REST, capacity)
    rest_shape = (device_count, 2 * block_count * share, channels // 2 * REST)
    fill = padded - layers
    gram = jnp.dot(sqrt_cov.T, sqrt_cov, precision=HIGHEST)
    gram = jnp.pad(gram, ((0, fill), (0, fill)))
    cov = jnp.pad(sqrt_cov.T, ((0, fill), (0, fill)))

    out = jax.ShapeDtypeStruct((GRID_BLK * BLOCK, layers), jnp.float32)
    vmem = pl.BlockSpec(memory_space=pltpu.VMEM)
    dma = pltpu.SemaphoreType.DMA
    return pl.pallas_call(
        functools.partial(cg_kernel, obs_count, chan_count),
        out_shape=(out, out),
        in_specs=[pl.BlockSpec(memory_space=pl.ANY)] + [vmem] * 3,
        out_specs=(vmem, vmem),
        scratch_shapes=[
            pltpu.VMEM((2, device_count, block_count, share, channels // 2, LANES), jnp.bfloat16),
            pltpu.VMEM(rest_shape, jnp.bfloat16),
            pltpu.VMEM(rest_shape, jnp.bfloat16),
            pltpu.VMEM((device_count * block_count * share * channels // 2, LANES), jnp.float32),
            pltpu.VMEM((rows, padded, LANES), jnp.float32),
            pltpu.VMEM((rows, LANES), jnp.float32),
            pltpu.VMEM((ITERS, device_count, 1, LANES), jnp.float32),
            pltpu.VMEM((2, device_count, 2 * GRID_BLK * share, layers), jnp.bfloat16),
            dma((2,)), dma((2,)), dma, dma,
            dma((2 * block_count,)),
            dma((ITERS,)),
            dma((ITERS,)),
            dma, dma,
        ],
        compiler_params=pltpu.CompilerParams(
            collective_id=0, has_side_effects=True, vmem_limit_bytes=50 * 1024 * 1024
        ),
    )(jacobian, rest, gram, cov)


def solution(mesh):
    device_count = mesh.shape["obs"] * mesh.shape["chan"]

    def plan(jacobian, departures, obs_weights, column_count, grid_block, sqrt_cov):
        capacity, channels, layers = jacobian.shape
        mine = capacity // device_count
        fits = (
            BLOCK % device_count == 0
            and mine == 8
            and 2 * mesh.shape["obs"] * mine == LANES
            and mesh.shape["chan"] % 2 == 0
            and channels % 32 == 0
            and LANES < layers <= LANES + REST - 4
        )
        chosen = shared_columns if fits else exchange_per_step
        return chosen(jacobian, departures, obs_weights, column_count, grid_block, sqrt_cov)

    in_specs = (P("obs", "chan", None), P("chan", "obs"), P("chan", "obs"), P("obs"), P("obs"), P())
    out_specs = (P("obs", None), P("obs", None))
    return jax.shard_map(plan, mesh=mesh, in_specs=in_specs, out_specs=out_specs, check_vma=False)
```

```python
import functools
import jax
import jax.numpy as jnp
from jax import lax
from jax.experimental import pallas as pl
from jax.experimental.pallas import tpu as pltpu
from jax.sharding import PartitionSpec as P

BLOCK = 128
ITERS = 5
GRID_BLK = 2
HIGHEST = lax.Precision.HIGHEST
MESH = pl.DeviceIdType.MESH


def block_terms(jac_part, weight_part, mask_part, predicted):
    scaled = (mask_part[:, None] * weight_part * predicted).astype(jnp.bfloat16)
    return lax.dot_general(
        jac_part, scaled, (((1,), (1,)), ((0,), (0,))), preferred_element_type=jnp.float32
    )


def forward_terms(jac_part, weight_part, mask_part, field_part):
    predicted = lax.dot_general(
        jac_part, field_part, (((2,), (1,)), ((0,), (0,))), preferred_element_type=jnp.float32
    )
    return block_terms(jac_part, weight_part, mask_part, predicted)


def exchange_per_step(jacobian, departures, obs_weights, column_count, grid_block, sqrt_cov):
    obs_count = lax.axis_size("obs")
    myself = lax.axis_index("obs")
    capacity, group_channels, layers = jacobian.shape
    block_count = capacity // BLOCK
    weight_cols = obs_weights.T
    depart_cols = departures.T
    observed = (jnp.arange(capacity, dtype=jnp.int32) < column_count[0]).astype(jnp.float32)
    every_id = lax.all_gather(grid_block, "obs", axis=0, tiled=True).reshape(obs_count, block_count)
    targets = jnp.arange(obs_count, dtype=jnp.int32)
    send_pick = (grid_block[None, :] // GRID_BLK == targets[:, None]).astype(jnp.float32)
    owned_here = every_id // GRID_BLK == myself
    places = every_id % GRID_BLK
    grid_index = jnp.arange(GRID_BLK, dtype=jnp.int32)
    take_pick = jnp.sum(
        ((places[None] == grid_index[:, None, None]) & owned_here[None]).astype(jnp.float32), axis=2
    )
    share_cols = BLOCK

    def local_terms(kernel_fn, inputs):
        return kernel_fn(jacobian, weight_cols, observed, inputs)

    def to_owners(terms):
        blocked = terms.reshape(block_count, BLOCK, layers)
        blocked = lax.psum(blocked, "chan")
        outgoing = jnp.dot(
            send_pick, blocked.reshape(block_count, -1), precision=lax.Precision.HIGHEST
        )
        incoming = lax.all_to_all(
            outgoing.reshape(obs_count, share_cols, layers),
            "obs",
            split_axis=0,
            concat_axis=0,
            tiled=True,
        )
        summed = jnp.dot(
            take_pick, incoming.reshape(obs_count, -1), precision=lax.Precision.HIGHEST
        )
        return summed.reshape(GRID_BLK, share_cols, layers)

    def spread(field):
        return jnp.dot(
            field.reshape(-1, layers), sqrt_cov, precision=lax.Precision.HIGHEST
        ).reshape(field.shape)

    def spread_back(field):
        flat = lax.dot_general(
            field.reshape(-1, layers),
            sqrt_cov,
            (((1,), (1,)), ((), ())),
            precision=lax.Precision.HIGHEST,
        )
        return flat.reshape(field.shape)

    def squared(values):
        partial_sum = jnp.sum(values * values)
        return lax.psum(partial_sum, "obs")

    residual = spread_back(to_owners(local_terms(block_terms, depart_cols)))
    control = jnp.zeros_like(residual)
    direction = residual
    norm_now = squared(residual)
    for iteration in range(ITERS):
        rounded = spread(direction).astype(jnp.bfloat16).reshape(GRID_BLK, -1)
        to_outgoing = jnp.dot(
            take_pick.T.astype(jnp.bfloat16), rounded, preferred_element_type=jnp.float32
        ).astype(jnp.bfloat16)
        to_incoming = lax.all_to_all(
            to_outgoing.reshape(obs_count, share_cols, layers),
            "obs",
            split_axis=0,
            concat_axis=0,
            tiled=True,
        )
        picked = jnp.dot(
            send_pick.T.astype(jnp.bfloat16),
            to_incoming.reshape(obs_count, -1),
            preferred_element_type=jnp.float32,
        )
        picked = picked.astype(jnp.bfloat16).reshape(block_count, share_cols, layers)
        fetched = picked.reshape(capacity, layers)
        image = direction + spread_back(to_owners(local_terms(forward_terms, fetched)))
        curvature_partial_sum = jnp.sum(direction * image)
        step_length = norm_now / lax.psum(curvature_partial_sum, "obs")
        control = control + step_length * direction
        residual = residual - step_length * image
        norm_next = squared(residual)
        direction = residual + norm_next / norm_now * direction
        norm_now = norm_next
    increment = spread(control)
    return (increment.reshape(-1, layers), residual.reshape(-1, layers))


LANES = 128
REST = 16
STRIDE = 11


def cg_kernel(
    obs_count, chan_count, jac_ref, rest_ref, gram_ref, cov_ref, increment_ref, residual_ref,
    got_ref, put_rest_ref, got_rest_ref, wide_ref, turned_ref, weight_ref, parts_ref, back_ref,
    jac_send, jac_recv, rest_send, rest_recv, own_sem, sum_send, sum_recv, back_send, back_recv
):
    device_count = obs_count * chan_count
    me = lax.axis_index("obs") * chan_count + lax.axis_index("chan")
    layers = increment_ref.shape[1]
    _, _, block_count, share, half_channels, _ = got_ref.shape
    channels = 2 * half_channels
    mine = block_count * share
    rows, padded, _ = turned_ref.shape
    lows = chan_count // 2
    grid_cols = GRID_BLK * obs_count * share
    piece = GRID_BLK * share

    def coords(target):
        return (target // chan_count, target % chan_count)

    barrier = pltpu.get_barrier_semaphore()

    def greet(offset, carry):
        pl.semaphore_signal(
            barrier, inc=1, device_id=coords((me + offset) % device_count), device_id_type=MESH
        )
        return carry

    lax.fori_loop(1, device_count, greet, 0)

    def own_part(part, block, target):
        return jac_ref.at[
            pl.ds(block * BLOCK + target * share, share), pl.ds(part * half_channels, half_channels), :
        ]

    own = [
        pltpu.make_async_copy(
            own_part(part, k, me), got_ref.at[part, me, k], own_sem.at[part * block_count + k]
        )
        for part in range(2)
        for k in range(block_count)
    ]
    for copy in own:
        copy.start()
    pl.semaphore_wait(barrier, device_count - 1)

    def send_columns(part):
        def send(offset, carry):
            target = (me + offset * STRIDE) % device_count
            for k in range(block_count):
                pltpu.make_async_remote_copy(
                    src_ref=own_part(part, k, target),
                    dst_ref=got_ref.at[part, me, k],
                    send_sem=jac_send.at[part],
                    recv_sem=jac_recv.at[part],
                    device_id=coords(target),
                    device_id_type=MESH,
                ).start()
            return carry

        lax.fori_loop(1, device_count, send, 0)

    def send_rest(offset, carry):
        target = (me + offset * STRIDE) % device_count
        pltpu.make_async_remote_copy(
            src_ref=put_rest_ref.at[target],
            dst_ref=got_rest_ref.at[me],
            send_sem=rest_send,
            recv_sem=rest_recv,
            device_id=coords(target),
            device_id_type=MESH,
        ).start()
        return carry

    send_columns(0)
    columns = block_count * BLOCK
    row = lax.broadcasted_iota(jnp.int32, (columns, columns), 0)
    column = lax.broadcasted_iota(jnp.int32, (columns, columns), 1)
    wanted = (row % mine) // share * BLOCK + row // mine * share + row % share
    order = jnp.where(column == wanted, 1.0, 0.0).astype(jnp.bfloat16)
    ordered = lax.dot_general(
        order, rest_ref[...], (((1,), (1,)), ((), ())), preferred_element_type=jnp.float32
    )
    width = half_channels * REST
    for part in range(2):
        strip = ordered[:, part * width : (part + 1) * width].astype(jnp.bfloat16)
        put_rest_ref[:, part * mine : (part + 1) * mine, :] = strip.reshape(device_count, mine, width)
    got_rest_ref[me] = put_rest_ref[me]
    lax.fori_loop(1, device_count, send_rest, 0)
    send_columns(1)
    for copy in own:
        copy.wait()

    def wait_others(ref, sem):
        others = ref.at[pl.ds(0, device_count - 1)]
        pltpu.make_async_copy(others, others, sem).wait()

    wait_others(got_rest_ref, rest_recv)
    wait_others(got_rest_ref, rest_send)

    def widen(part):
        def step(source, carry):
            block = got_ref[part, source].astype(jnp.float32).reshape(-1, LANES)
            wide_ref[pl.ds(source * mine * half_channels, mine * half_channels), :] = block
            return carry

        lax.fori_loop(0, device_count, step, 0)

    def source_of(half, obs, low):
        return obs * chan_count + half * lows + low

    def turn_half(part, low):
        first = low * channels + part * half_channels

        def turn(n, carry):
            picked = [
                wide_ref[
                    pl.ds(source_of(half, obs, low) * mine * half_channels + n, mine, stride=half_channels), :
                ]
                for half in range(2)
                for obs in range(obs_count)
            ]
            turned_ref[first + n, 0:LANES, :] = jnp.concatenate(picked, axis=0).T
            return carry

        lax.fori_loop(0, half_channels, turn, 0, unroll=2)
        picked = [
            got_rest_ref[source_of(half, obs, low)].astype(jnp.float32)[part * mine : (part + 1) * mine]
            for half in range(2)
            for obs in range(obs_count)
        ]
        flipped = jnp.concatenate(picked, axis=0).T
        for n in range(half_channels):
            turned_ref[first + n, LANES:padded, :] = flipped[n * REST : (n + 1) * REST]

    for part in range(2):
        others = got_ref.at[part, pl.ds(0, device_count - 1)]
        pltpu.make_async_copy(others, others, jac_recv.at[part]).wait()
        pltpu.make_async_copy(others, others, jac_send.at[part]).wait()
        widen(part)
        for low in range(lows):
            turn_half(part, low)

    def dot(a, b):
        return jnp.dot(a, b, precision=HIGHEST, preferred_element_type=jnp.float32)

    ids = turned_ref[0, layers + 3 : layers + 4, :].astype(jnp.int32)
    lane = lax.broadcasted_iota(jnp.int32, (grid_cols, LANES), 1)
    spot = lax.broadcasted_iota(jnp.int32, (grid_cols, LANES), 0)
    pick = (spot == ids * share + lane % share).astype(jnp.float32)

    def times(a, b, b_dim):
        total = None
        for _ in range(3):
            part = a.astype(jnp.bfloat16)
            a = a - part.astype(jnp.float32)
            product = lax.dot_general(
                part, b, (((1,), (b_dim,)), ((), ())), preferred_element_type=jnp.float32
            )
            total = product if total is None else total + product
        return total

    picked_bf16 = pick.astype(jnp.bfloat16)
    shared = lax.dot_general(
        picked_bf16, picked_bf16, (((0,), (0,)), ((), ())), preferred_element_type=jnp.float32
    )
    copies = jnp.sum(shared, axis=0, keepdims=True)
    shared = shared.astype(jnp.bfloat16)

    def collect(terms):
        return times(terms, shared, 0)

    def source_step(n, acc):
        kernel = turned_ref[n]
        weight_ref[pl.ds(n, 1), :] = kernel[layers : layers + 1] + kernel[layers + 1 : layers + 2]
        return acc + kernel * kernel[layers + 2 : layers + 3]

    zero = jnp.zeros((padded, LANES), jnp.float32)
    residual = collect(lax.fori_loop(0, rows, source_step, zero, unroll=4))

    def normal(field, spread):
        def normal_step(n, acc):
            kernel = turned_ref[n]
            predicted = jnp.sum(kernel * spread, axis=0, keepdims=True)
            return acc + kernel * (predicted * weight_ref[pl.ds(n, 1), :])

        return field + collect(lax.fori_loop(0, rows, normal_step, zero, unroll=4))

    share_of = 1.0 / copies
    spread = dot(gram_ref[...], residual)
    applied = normal(residual, spread)
    control = direction = image = spread_image = image_applied = None
    norm_last = step_last = None
    for step in range(ITERS):
        norm_part = jnp.sum(residual * spread, axis=0, keepdims=True) * share_of
        curve_part = jnp.sum(applied * spread, axis=0, keepdims=True) * share_of
        norm_part = jnp.sum(norm_part, axis=1, keepdims=True)
        curve_part = jnp.sum(curve_part, axis=1, keepdims=True)
        place = lax.broadcasted_iota(jnp.int32, (1, LANES), 1)
        parts_ref[step, me] = jnp.where(place == 0, norm_part, jnp.where(place == 1, curve_part, 0.0))

        def send_sum(offset, carry, step=step):
            pltpu.make_async_remote_copy(
                src_ref=parts_ref.at[step, me],
                dst_ref=parts_ref.at[step, me],
                send_sem=sum_send.at[step],
                recv_sem=sum_recv.at[step],
                device_id=coords((me + offset) % device_count),
                device_id_type=MESH,
            ).start()
            return carry

        lax.fori_loop(1, device_count, send_sum, 0)
        last = step == ITERS - 1
        if not last:
            next_spread = dot(gram_ref[...], applied)
            next_applied = normal(applied, next_spread)
        others = parts_ref.at[step, pl.ds(0, device_count - 1)]
        pltpu.make_async_copy(others, others, sum_recv.at[step]).wait()
        pltpu.make_async_copy(others, others, sum_send.at[step]).wait()
        total = jnp.sum(parts_ref[step], axis=0)
        norm_now = jnp.sum(jnp.where(place == 0, total, 0.0), axis=1, keepdims=True)
        curve = jnp.sum(jnp.where(place == 1, total, 0.0), axis=1, keepdims=True)
        if step == 0:
            length = norm_now / curve
            direction, image = residual, applied
            spread_image, image_applied = next_spread, next_applied
            control = length * direction
        else:
            ratio = norm_now / norm_last
            length = norm_now / (curve - ratio * norm_now / step_last)
            direction = residual + ratio * direction
            image = applied + ratio * image
            if not last:
                spread_image = next_spread + ratio * spread_image
                image_applied = next_applied + ratio * image_applied
            control = control + length * direction
        residual = residual - length * image
        if not last:
            spread = spread - length * spread_image
            applied = applied - length * image_applied
        norm_last, step_last = norm_now, length
    control = times(control * share_of, picked_bf16, 1)
    residual = times(residual * share_of, picked_bf16, 1)

    def flip_dot(a, b):
        return lax.dot_general(
            a, b, (((0,), (0,)), ((), ())), precision=HIGHEST, preferred_element_type=jnp.float32
        )

    outs = (flip_dot(control, gram_ref[...]), flip_dot(residual, cov_ref[...]))
    out_stage, landed = back_ref.at[0], back_ref.at[1]
    for owner in range(obs_count):
        pieces = [value[owner * piece : (owner + 1) * piece, :layers] for value in outs]
        out_stage[owner * chan_count, :, :] = jnp.concatenate(pieces, axis=0).astype(jnp.bfloat16)
    landed[me] = out_stage[(me // chan_count) * chan_count]

    def send_back(offset, carry):
        target = (me + offset) % device_count
        pltpu.make_async_remote_copy(
            src_ref=out_stage.at[(target // chan_count) * chan_count],
            dst_ref=landed.at[me],
            send_sem=back_send,
            recv_sem=back_recv,
            device_id=coords(target),
            device_id_type=MESH,
        ).start()
        return carry

    lax.fori_loop(1, device_count, send_back, 0)
    others = landed.at[pl.ds(0, device_count - 1)]
    pltpu.make_async_copy(others, others, back_recv).wait()
    pltpu.make_async_copy(others, others, back_send).wait()
    for source in range(device_count):
        block_rows = landed[source].astype(jnp.float32)
        for which, out_ref in enumerate((increment_ref, residual_ref)):
            for block in range(GRID_BLK):
                first = block * BLOCK + source * share
                taken = which * piece + block * share
                out_ref[first : first + share, :] = block_rows[taken : taken + share]


def shared_columns(jacobian, departures, obs_weights, column_count, grid_block, sqrt_cov):
    obs_count, chan_count = lax.axis_size("obs"), lax.axis_size("chan")
    device_count = obs_count * chan_count
    capacity, channels, layers = jacobian.shape
    block_count = capacity // BLOCK
    share = BLOCK // device_count
    padded = LANES + REST
    rows = channels * chan_count // 2

    observed = (jnp.arange(capacity, dtype=jnp.int32) < column_count[0]).astype(jnp.float32)
    weight = observed[None, :] * obs_weights
    weight_high = weight.astype(jnp.bfloat16)
    weight_low = (weight - weight_high.astype(jnp.float32)).astype(jnp.bfloat16)
    source = (weight * departures).astype(jnp.bfloat16)
    ids = jnp.broadcast_to(jnp.repeat(grid_block, BLOCK)[None, :], weight.shape)
    extra = jnp.stack([weight_high, weight_low, source, ids.astype(jnp.bfloat16)], axis=1)
    rest = jnp.concatenate([jacobian[:, :, LANES:].transpose(1, 2, 0), extra], axis=1)
    rest = jnp.pad(rest, ((0, 0), (0, padded - layers - 4), (0, 0)))
    rest = rest.reshape(channels * REST, capacity)
    rest_shape = (device_count, 2 * block_count * share, channels // 2 * REST)
    fill = padded - layers
    gram = jnp.dot(sqrt_cov.T, sqrt_cov, precision=HIGHEST)
    gram = jnp.pad(gram, ((0, fill), (0, fill)))
    cov = jnp.pad(sqrt_cov.T, ((0, fill), (0, fill)))

    out = jax.ShapeDtypeStruct((GRID_BLK * BLOCK, layers), jnp.float32)
    vmem = pl.BlockSpec(memory_space=pltpu.VMEM)
    dma = pltpu.SemaphoreType.DMA
    return pl.pallas_call(
        functools.partial(cg_kernel, obs_count, chan_count),
        out_shape=(out, out),
        in_specs=[pl.BlockSpec(memory_space=pl.ANY)] + [vmem] * 3,
        out_specs=(vmem, vmem),
        scratch_shapes=[
            pltpu.VMEM((2, device_count, block_count, share, channels // 2, LANES), jnp.bfloat16),
            pltpu.VMEM(rest_shape, jnp.bfloat16),
            pltpu.VMEM(rest_shape, jnp.bfloat16),
            pltpu.VMEM((device_count * block_count * share * channels // 2, LANES), jnp.float32),
            pltpu.VMEM((rows, padded, LANES), jnp.float32),
            pltpu.VMEM((rows, LANES), jnp.float32),
            pltpu.VMEM((ITERS, device_count, 1, LANES), jnp.float32),
            pltpu.VMEM((2, device_count, 2 * GRID_BLK * share, layers), jnp.bfloat16),
            dma((2,)), dma((2,)), dma, dma,
            dma((2 * block_count,)),
            dma((ITERS,)),
            dma((ITERS,)),
            dma, dma,
        ],
        compiler_params=pltpu.CompilerParams(
            collective_id=0, has_side_effects=True, vmem_limit_bytes=50 * 1024 * 1024
        ),
    )(jacobian[:, :, :LANES], rest, gram, cov)


def solution(mesh):
    device_count = mesh.shape["obs"] * mesh.shape["chan"]

    def plan(jacobian, departures, obs_weights, column_count, grid_block, sqrt_cov):
        capacity, channels, layers = jacobian.shape
        mine = capacity // device_count
        fits = (
            BLOCK % device_count == 0
            and mine == 8
            and 2 * mesh.shape["obs"] * mine == LANES
            and mesh.shape["chan"] % 2 == 0
            and channels % 32 == 0
            and LANES < layers <= LANES + REST - 4
        )
        chosen = shared_columns if fits else exchange_per_step
        return chosen(jacobian, departures, obs_weights, column_count, grid_block, sqrt_cov)

    in_specs = (P("obs", "chan", None), P("chan", "obs"), P("chan", "obs"), P("obs"), P("obs"), P())
    out_specs = (P("obs", None), P("obs", None))
    return jax.shard_map(plan, mesh=mesh, in_specs=in_specs, out_specs=out_specs, check_vma=False)
```
